32 devices in a mesh: dp: 2 (over x), tp: 16 (over y, z, core).
Axes of the slice: x: 2, y: 2, z: 4, core: 2. Of those that a mesh axis runs over, the one named last changes fastest.
Arguments:
- x: bfloat16 [5120, 7168], P(('dp', 'tp')), parts along dimension 0
- w_gate: bfloat16 [7168, 20480], P(None, 'tp')
- w_up: bfloat16 [7168, 20480], P(None, 'tp')
- w_down: bfloat16 [20480, 7168], P('tp')
Outputs:
- output: bfloat16 [5120, 7168], P(('dp', 'tp')), parts along dimension 0
There are 2 independent parts. The reference program is written for one: setup_inputs(seed, part) draws one part's arguments, and reference() takes and returns one part's arrays. A program takes and returns all parts, laid end to end along the dimension named above; an argument that names none is the same for every part.
All inputs are finite; a program needn't handle non-finite values.
Results may differ from the reference program's by a relative error of at most 0.016.
Values are sent between devices in bfloat16 or wider.
A program may use at most 2 GiB of HBM per device.

```python
import jax
import jax.numpy as jnp

ROWS = 2560
D = 7168
FF = 20480


def setup_inputs(seed: int = 0, part: int = 0) -> dict:
    kx, kg, ku, kd = jax.random.split(jax.random.key(seed), 4)
    drawn = {
        "x": jax.random.normal(jax.random.fold_in(kx, part), (ROWS, D), jnp.float32),
        "w_gate": jax.random.normal(kg, (D, FF), jnp.float32) * D**-0.5,
        "w_up": jax.random.normal(ku, (D, FF), jnp.float32) * D**-0.5,
        "w_down": jax.random.normal(kd, (FF, D), jnp.float32) * FF**-0.5,
    }
    return {k: v.astype(jnp.bfloat16) for k, v in drawn.items()}


def reference(x, w_gate, w_up, w_down):
    gate = jnp.dot(x, w_gate, preferred_element_type=jnp.float32)
    up = jnp.dot(x, w_up, preferred_element_type=jnp.float32)
    hidden = (jax.nn.silu(gate) * up).astype(jnp.bfloat16)
    return jnp.dot(hidden, w_down, preferred_element_type=jnp.float32).astype(jnp.bfloat16)
```

```python
import jax
import jax.numpy as jnp
from jax import lax
from jax.experimental import pallas as pl
from jax.experimental.pallas import tpu as pltpu
from jax.sharding import PartitionSpec as P

MESH = pl.DeviceIdType.MESH
F32 = jnp.float32
BF16 = jnp.bfloat16
RING = 8
TF = 256
TN = 1024


def chip_at(place):
    y = lax.div(place, 4)
    along = lax.rem(place, 4)
    return 4 * y + along + y * (3 - 2 * along)


def kernel(x_ref, wg_ref, wu_ref, wd_ref, y_ref, xg_ref, xbuf, wgbuf, wubuf, wdbuf, hid, acc, rs, d2d, pbuf, sbuf,
           ag_send, ag_recv, xd_send, xd_recv, rs_send, rs_recv, dd_send, dd_recv, x_sem, wgu_sem, wd_sem, y_sem):
    rows = x_ref.shape[0]
    half = rows // 2
    nf = wg_ref.shape[1] // TF
    nn = wd_ref.shape[1] // TN
    me = lax.axis_index("tp")
    chip = lax.div(me, 2)
    core = lax.rem(me, 2)
    y, z = lax.div(chip, 4), lax.rem(chip, 4)
    place = z + y * (7 - 2 * z)
    nxt = chip_at(lax.rem(place + 1, RING)) * 2 + core
    prv = chip_at(lax.rem(place + RING - 1, RING)) * 2 + core
    partner = chip * 2 + 1 - core
    to = (nxt, prv)

    barrier = pltpu.get_barrier_semaphore()
    for other in (nxt, prv, partner):
        pl.semaphore_signal(barrier, inc=1, device_id={"tp": other}, device_id_type=MESH)
    pl.semaphore_wait(barrier, 3)

    def part(d):
        return pl.ds(d * half, half)

    def remote(src, dst, send, recv, dev):
        return pltpu.make_async_remote_copy(
            src_ref=src, dst_ref=dst, send_sem=send, recv_sem=recv, device_id={"tp": dev}, device_id_type=MESH)

    def ag(s, d, first=False):
        src = x_ref.at[part(d)] if first else xg_ref.at[s - 1, part(d)]
        return remote(src, xg_ref.at[s, part(d)], ag_send.at[s, d], ag_recv.at[s, d], to[d])

    def xd(s, own=False):
        src = x_ref if own else xg_ref.at[s - 1, pl.ds(0, rows)]
        return remote(src, xg_ref.at[s - 1, pl.ds(rows, rows)], xd_send.at[s - 1], xd_recv.at[s - 1], partner)

    def rsc(s, n, d):
        return remote(sbuf.at[lax.rem(s, 2), n, part(d)], rs.at[lax.rem(s + 1, 3), n, part(d)],
                      rs_send.at[lax.rem(s, 2), n, d], rs_recv.at[lax.rem(s + 1, 3), n, d], to[d])

    def rs_in(s, n, d):
        return remote(sbuf.at[0, n, part(d)], rs.at[lax.rem(s, 3), n, part(d)],
                      rs_send.at[0, n, d], rs_recv.at[lax.rem(s, 3), n, d], to[d])

    def dd(n):
        return remote(pbuf.at[n], d2d.at[n], dd_send.at[n], dd_recv.at[n], partner)

    def wgu(i):
        t, slot = lax.rem(i, nf), lax.rem(i, 2)
        cols = pl.ds(pl.multiple_of(t * TF, TF), TF)
        return (pltpu.make_async_copy(wg_ref.at[:, cols], wgbuf.at[slot], wgu_sem.at[slot, 0]),
                pltpu.make_async_copy(wu_ref.at[:, cols], wubuf.at[slot], wgu_sem.at[slot, 1]))

    def wdn(j):
        n, slot = lax.rem(j, nn), lax.rem(j, 2)
        cols = pl.ds(pl.multiple_of(n * TN, TN), TN)
        return pltpu.make_async_copy(wd_ref.at[:, cols], wdbuf.at[slot], wd_sem.at[slot])

    def y_out(n):
        cols = pl.ds(pl.multiple_of(n * TN, TN), TN)
        return pltpu.make_async_copy(sbuf.at[0, n], y_ref.at[:, cols], y_sem.at[n])

    for d in (0, 1):
        ag(0, d, first=True).start()
    for copy in wgu(0):
        copy.start()
    wdn(0).start()

    def step(s, carry):
        @pl.when(s < RING)
        def _():
            for d in (0, 1):
                ag(s - 1, d, first=True).wait_recv()

                @pl.when(s < RING - 1)
                def _():
                    ag(s, d).start()
            xd(s).start()
            pltpu.make_async_copy(xg_ref.at[s - 1, pl.ds(0, rows)], xbuf.at[pl.ds(0, rows)], x_sem.at[0]).start()

        @pl.when(s == RING)
        def _():
            xd(s, own=True).start()
            pltpu.make_async_copy(x_ref, xbuf.at[pl.ds(0, rows)], x_sem.at[0]).start()

        xd(s).wait_recv()
        theirs = pltpu.make_async_copy(
            xg_ref.at[s - 1, pl.ds(rows, rows)], xbuf.at[pl.ds(rows, rows)], x_sem.at[1])
        theirs.start()
        pltpu.make_async_copy(xg_ref.at[s - 1, pl.ds(0, rows)], xbuf.at[pl.ds(0, rows)], x_sem.at[0]).wait()
        theirs.wait()

        def gate_up(t, carry):
            i = (s - 1) * nf + t

            @pl.when(i + 1 < RING * nf)
            def _():
                for copy in wgu(i + 1):
                    copy.start()
            for copy in wgu(i):
                copy.wait()
            slot = lax.rem(i, 2)
            gate = jnp.dot(xbuf[...], wgbuf[slot], preferred_element_type=F32)
            up = jnp.dot(xbuf[...], wubuf[slot], preferred_element_type=F32)
            hid[t] = (jax.nn.silu(gate) * up).astype(BF16)
            return carry

        lax.fori_loop(0, nf, gate_up, 0)

        def combine(n):
            k = lax.rem(n, 2)

            @pl.when(s > 1)
            def _():
                for d in (0, 1):
                    rs_in(s, n, d).wait_recv()
                acc[k] = acc[k] + rs[lax.rem(s, 3), n].astype(F32)

            @pl.when((s > 2))
            def _():
                for d in (0, 1):
                    rsc(s - 2, n, d).wait_send()
            dd(n).wait_recv()
            sbuf[lax.rem(s, 2), n] = (acc[k] + d2d[n].astype(F32)).astype(BF16)

            @pl.when(s < RING)
            def _():
                for d in (0, 1):
                    rsc(s, n, d).start()

            @pl.when(s == RING)
            def _():
                y_out(n).start()

        def down(n, carry):
            j = (s - 1) * nn + n

            @pl.when(j + 1 < RING * nn)
            def _():
                wdn(j + 1).start()
            wdn(j).wait()
            slot = lax.rem(j, 2)
            term = jnp.dot(hid[0], wdbuf[slot, 0:TF], preferred_element_type=F32)
            for t in range(1, nf):
                term += jnp.dot(hid[t], wdbuf[slot, t * TF:(t + 1) * TF], preferred_element_type=F32)
            acc[lax.rem(n, 2)] = term[:rows]

            @pl.when(s > 1)
            def _():
                dd(n).wait_send()
            pbuf[n] = term[rows:].astype(BF16)
            dd(n).start()

            @pl.when(n > 0)
            def _():
                combine(n - 1)
            return carry

        lax.fori_loop(0, nn, down, 0)
        combine(nn - 1)
        return carry

    lax.fori_loop(1, RING + 1, step, 0)

    def drain(n, carry):
        y_out(n).wait()
        dd(n).wait_send()
        for d in (0, 1):
            rsc(RING - 1, n, d).wait_send()
        return carry

    lax.fori_loop(0, nn, drain, 0)
    for s in range(RING):
        xd(s + 1).wait_send()
        if s < RING - 1:
            for d in (0, 1):
                ag(s, d, first=s == 0).wait_send()


def solution(mesh):
    def step(x, w_gate, w_up, w_down):
        rows, dim = x.shape
        ff = w_gate.shape[1]
        nn = dim // TN
        hbm = pl.BlockSpec(memory_space=pl.ANY)
        dma = pltpu.SemaphoreType.DMA
        out, _ = pl.pallas_call(
            kernel,
            out_shape=(
                jax.ShapeDtypeStruct((rows, dim), BF16),
                jax.ShapeDtypeStruct((RING, 2 * rows, dim), BF16),
            ),
            in_specs=[hbm] * 4,
            out_specs=(hbm, hbm),
            scratch_shapes=[
                pltpu.VMEM((2 * rows, dim), BF16),
                pltpu.VMEM((2, dim, TF), BF16),
                pltpu.VMEM((2, dim, TF), BF16),
                pltpu.VMEM((2, ff, TN), BF16),
                pltpu.VMEM((ff // TF, 2 * rows, TF), BF16),
                pltpu.VMEM((2, rows, TN), F32),
                pltpu.VMEM((3, nn, rows, TN), BF16),
                pltpu.VMEM((nn, rows, TN), BF16),
                pltpu.VMEM((nn, rows, TN), BF16),
                pltpu.VMEM((2, nn, rows, TN), BF16),
                dma((RING, 2)), dma((RING, 2)),
                dma((RING,)), dma((RING,)),
                dma((2, nn, 2)), dma((3, nn, 2)),
                dma((nn,)), dma((nn,)),
                dma((2,)), dma((2, 2)), dma((2,)), dma((nn,)),
            ],
            compiler_params=pltpu.CompilerParams(
                collective_id=0, has_side_effects=True, vmem_limit_bytes=62 * 1024 * 1024),
        )(x, w_gate, w_up, w_down)
        return out

    return jax.shard_map(
        step,
        mesh=mesh,
        in_specs=(P(("dp", "tp"), None), P(None, "tp"), P(None, "tp"), P("tp", None)),
        out_specs=P(("dp", "tp"), None),
        check_vma=False,
    )
```

```python
import jax
import jax.numpy as jnp
from jax import lax
from jax.experimental import pallas as pl
from jax.experimental.pallas import tpu as pltpu
from jax.sharding import PartitionSpec as P

MESH = pl.DeviceIdType.MESH
F32 = jnp.float32
BF16 = jnp.bfloat16
RING = 8
TF = 256
TN = 1024
EARLY = 2
SLOTS = 4


def chip_at(place):
    y = lax.div(place, 4)
    along = lax.rem(place, 4)
    return 4 * y + along + y * (3 - 2 * along)


def kernel(x_ref, wg_ref, wu_ref, wd_ref, y_ref, xg_ref, xbuf, wgbuf, wubuf, wdbuf, hid, acc, own, rs, d2d, pbuf, sbuf,
           ag_send, ag_recv, xd_send, xd_recv, rs_send, rs_recv, dd_send, dd_recv, x_sem, wgu_sem, wd_sem, y_sem):
    rows = x_ref.shape[0]
    half = rows // 2
    nf = wg_ref.shape[1] // TF
    nn = wd_ref.shape[1] // TN
    me = lax.axis_index("tp")
    chip = lax.div(me, 2)
    core = lax.rem(me, 2)
    y, z = lax.div(chip, 4), lax.rem(chip, 4)
    place = z + y * (7 - 2 * z)
    nxt = chip_at(lax.rem(place + 1, RING)) * 2 + core
    prv = chip_at(lax.rem(place + RING - 1, RING)) * 2 + core
    partner = chip * 2 + 1 - core
    to = (nxt, prv)

    barrier = pltpu.get_barrier_semaphore()
    for other in (nxt, prv, partner):
        pl.semaphore_signal(barrier, inc=1, device_id={"tp": other}, device_id_type=MESH)
    pl.semaphore_wait(barrier, 3)

    def part(d):
        return pl.ds(d * half, half)

    def remote(src, dst, send, recv, dev):
        return pltpu.make_async_remote_copy(
            src_ref=src, dst_ref=dst, send_sem=send, recv_sem=recv, device_id={"tp": dev}, device_id_type=MESH)

    def ag(s, d, p, first=False):
        piece = pl.ds(d * half + p * (half // 2), half // 2)
        src = x_ref.at[piece] if first else xg_ref.at[s - 1, piece]
        k = d * 2 + p
        return remote(src, xg_ref.at[s, piece], ag_send.at[s, k], ag_recv.at[s, k], to[d])

    def xd(s, own=False):
        k = lax.rem(s + RING - 1, RING)
        src = x_ref if own else xg_ref.at[k, pl.ds(0, rows)]
        return remote(src, xg_ref.at[k, pl.ds(rows, rows)], xd_send.at[k], xd_recv.at[k], partner)

    def rsc(s, n, d):
        return remote(sbuf.at[lax.rem(s, 2), n, part(d)], rs.at[lax.rem(s + 1, SLOTS), n, part(d)],
                      rs_send.at[lax.rem(s, 2), n, d], rs_recv.at[lax.rem(s + 1, SLOTS), n, d], to[d])

    def rs_in(s, n, d):
        return remote(sbuf.at[0, n, part(d)], rs.at[lax.rem(s, SLOTS), n, part(d)],
                      rs_send.at[0, n, d], rs_recv.at[lax.rem(s, SLOTS), n, d], to[d])

    def dd(s, n):
        slot = lax.rem(s, 2)
        return remote(pbuf.at[n], d2d.at[slot, n], dd_send.at[n], dd_recv.at[slot, n], partner)

    def wgu(i):
        t, slot = lax.rem(i, nf), lax.rem(i, 2)
        cols = pl.ds(pl.multiple_of(t * TF, TF), TF)
        return (pltpu.make_async_copy(wg_ref.at[:, cols], wgbuf.at[slot], wgu_sem.at[slot, 0]),
                pltpu.make_async_copy(wu_ref.at[:, cols], wubuf.at[slot], wgu_sem.at[slot, 1]))

    def wdn(j):
        n, slot = lax.rem(j, nn), lax.rem(j, 2)
        cols = pl.ds(pl.multiple_of(n * TN, TN), TN)
        return pltpu.make_async_copy(wd_ref.at[:, cols], wdbuf.at[slot], wd_sem.at[slot])

    def y_out(n):
        cols = pl.ds(pl.multiple_of(n * TN, TN), TN)
        return pltpu.make_async_copy(sbuf.at[0, n], y_ref.at[:, cols], y_sem.at[n])

    for p in (0, 1):
        for d in (0, 1):
            ag(0, d, p, first=True).start()
    for copy in wgu(0):
        copy.start()
    wdn(0).start()

    def x_mine(s):
        return pltpu.make_async_copy(xg_ref.at[s - 1, pl.ds(0, rows)], xbuf.at[pl.ds(0, rows)], x_sem.at[0])

    def x_theirs(s):
        k = lax.rem(s + RING - 1, RING)
        return pltpu.make_async_copy(xg_ref.at[k, pl.ds(rows, rows)], xbuf.at[pl.ds(rows, rows)], x_sem.at[1])

    def onward(s, p):
        for d in (0, 1):
            ag(s - 1, d, p, first=True).wait_recv()

            @pl.when(s < RING - 1)
            def _():
                ag(s, d, p).start()

    def arrive(s):
        @pl.when(s > EARLY)
        def _():
            onward(s, 0)
        onward(s, 1)
        xd(s).start()
        x_mine(s).start()

    xd(0, own=True).start()
    pltpu.make_async_copy(x_ref, xbuf.at[pl.ds(0, rows)], x_sem.at[0]).start()
    xd(0, own=True).wait_recv()
    x_theirs(0).start()

    def step(s, carry):
        pltpu.make_async_copy(x_ref, xbuf.at[pl.ds(0, rows)], x_sem.at[0]).wait()
        x_theirs(s).wait()

        def gate_up(t, carry):
            i = s * nf + t

            @pl.when(i + 1 < RING * nf)
            def _():
                for copy in wgu(i + 1):
                    copy.start()
            for copy in wgu(i):
                copy.wait()
            slot = lax.rem(i, 2)

            @pl.when((s < EARLY) & (t == nf - 3))
            def _():
                onward(s + 1, 0)
            gate = jnp.dot(xbuf[...], wgbuf[slot], preferred_element_type=F32)
            up = jnp.dot(xbuf[...], wubuf[slot], preferred_element_type=F32)
            hid[t] = (jax.nn.silu(gate) * up).astype(BF16)
            return carry

        lax.fori_loop(0, nf, gate_up, 0)

        def combine(n):
            k = lax.rem(n, 2)
            dd(s, n).wait_recv()

            @pl.when(s == 0)
            def _():
                own[n] = acc[k] + d2d[lax.rem(s, 2), n].astype(F32)

            @pl.when(s > 1)
            def _():
                for d in (0, 1):
                    rs_in(s, n, d).wait_recv()
                acc[k] = acc[k] + rs[lax.rem(s, SLOTS), n].astype(F32)

            @pl.when(s > 2)
            def _():
                for d in (0, 1):
                    rsc(s - 2, n, d).wait_send()

            @pl.when(s > 0)
            def _():
                sbuf[lax.rem(s, 2), n] = (acc[k] + d2d[lax.rem(s, 2), n].astype(F32)).astype(BF16)
                for d in (0, 1):
                    rsc(s, n, d).start()

        def down(n, carry):
            j = s * nn + n

            @pl.when(j + 1 < RING * nn)
            def _():
                wdn(j + 1).start()
            wdn(j).wait()
            slot = lax.rem(j, 2)
            term = jnp.dot(hid[0], wdbuf[slot, 0:TF], preferred_element_type=F32)
            for t in range(1, nf):
                term += jnp.dot(hid[t], wdbuf[slot, t * TF:(t + 1) * TF], preferred_element_type=F32)
            acc[lax.rem(n, 2)] = term[:rows]

            @pl.when(s > 0)
            def _():
                dd(s, n).wait_send()
            pbuf[n] = term[rows:].astype(BF16)
            dd(s, n).start()

            @pl.when(n > 0)
            def _():
                combine(n - 1)

            @pl.when((s < RING - 1) & (n == nn - 3))
            def _():
                xd(s + 1).wait_recv()
                x_theirs(s + 1).start()
            return carry

        @pl.when(s < RING - 1)
        def _():
            arrive(s + 1)

        lax.fori_loop(0, nn, down, 0)
        combine(nn - 1)
        return carry

    lax.fori_loop(0, RING, step, 0)

    def finish(n, carry):
        for d in (0, 1):
            rsc(RING - 2, n, d).wait_send()
            rs_in(RING, n, d).wait_recv()
        sbuf[0, n] = (own[n] + rs[RING % SLOTS, n].astype(F32)).astype(BF16)
        y_out(n).start()
        return carry

    lax.fori_loop(0, nn, finish, 0)

    def drain(n, carry):
        y_out(n).wait()
        dd(0, n).wait_send()
        for d in (0, 1):
            rsc(RING - 1, n, d).wait_send()
        return carry

    lax.fori_loop(0, nn, drain, 0)
    for s in range(RING):
        xd(s).wait_send()
        if s < RING - 1:
            for d in (0, 1):
                for p in (0, 1):
                    ag(s, d, p, first=s == 0).wait_send()


def solution(mesh):
    def step(x, w_gate, w_up, w_down):
        rows, dim = x.shape
        ff = w_gate.shape[1]
        nn = dim // TN
        hbm = pl.BlockSpec(memory_space=pl.ANY)
        dma = pltpu.SemaphoreType.DMA
        out, _ = pl.pallas_call(
            kernel,
            out_shape=(
                jax.ShapeDtypeStruct((rows, dim), BF16),
                jax.ShapeDtypeStruct((RING, 2 * rows, dim), BF16),
            ),
            in_specs=[hbm] * 4,
            out_specs=(hbm, hbm),
            scratch_shapes=[
                pltpu.VMEM((2 * rows, dim), BF16),
                pltpu.VMEM((2, dim, TF), BF16),
                pltpu.VMEM((2, dim, TF), BF16),
                pltpu.VMEM((2, ff, TN), BF16),
                pltpu.VMEM((ff // TF, 2 * rows, TF), BF16),
                pltpu.VMEM((2, rows, TN), F32),
                pltpu.VMEM((nn, rows, TN), F32),
                pltpu.VMEM((SLOTS, nn, rows, TN), BF16),
                pltpu.VMEM((2, nn, rows, TN), BF16),
                pltpu.VMEM((nn, rows, TN), BF16),
                pltpu.VMEM((2, nn, rows, TN), BF16),
                dma((RING, 4)), dma((RING, 4)),
                dma((RING,)), dma((RING,)),
                dma((2, nn, 2)), dma((SLOTS, nn, 2)),
                dma((nn,)), dma((2, nn)),
                dma((2,)), dma((2, 2)), dma((2,)), dma((nn,)),
            ],
            compiler_params=pltpu.CompilerParams(
                collective_id=0, has_side_effects=True, vmem_limit_bytes=62 * 1024 * 1024),
        )(x, w_gate, w_up, w_down)
        return out

    return jax.shard_map(
        step,
        mesh=mesh,
        in_specs=(P(("dp", "tp"), None), P(None, "tp"), P(None, "tp"), P("tp", None)),
        out_specs=P(("dp", "tp"), None),
        check_vma=False,
    )
```

```python
import jax
import jax.numpy as jnp
from jax import lax
from jax.experimental import pallas as pl
from jax.experimental.pallas import tpu as pltpu
from jax.sharding import PartitionSpec as P

MESH = pl.DeviceIdType.MESH
F32 = jnp.float32
BF16 = jnp.bfloat16
RING = 8
TF = 256
TN = 1024
EARLY = 2
LATE = 2
SLOTS = 4


def chip_at(place):
    y = lax.div(place, 4)
    along = lax.rem(place, 4)
    return 4 * y + along + y * (3 - 2 * along)


def kernel(x_ref, wg_ref, wu_ref, wd_ref, y_ref, xg_ref, xbuf, wgbuf, wubuf, wdbuf, hid, acc, own, rs, qb, d2d, pbuf, sbuf,
           ag_send, ag_recv, xd_send, xd_recv, rs_send, rs_recv, dd_send, dd_recv, x_sem, wgu_sem, wd_sem, y_sem, cs_send, bk_send, q_recv):
    rows = x_ref.shape[0]
    half = rows // 2
    nf = wg_ref.shape[1] // TF
    nn = wd_ref.shape[1] // TN
    me = lax.axis_index("tp")
    chip = lax.div(me, 2)
    core = lax.rem(me, 2)
    y, z = lax.div(chip, 4), lax.rem(chip, 4)
    place = z + y * (7 - 2 * z)
    nxt = chip_at(lax.rem(place + 1, RING)) * 2 + core
    prv = chip_at(lax.rem(place + RING - 1, RING)) * 2 + core
    partner = chip * 2 + 1 - core
    to = (nxt, prv)
    cross = chip_at(RING - 1 - place) * 2 + core
    role = lax.rem(place, 4)
    rho = (role, 3 - role)
    mid = (role == 1) | (role == 2)

    barrier = pltpu.get_barrier_semaphore()
    for other in (nxt, prv, partner):
        pl.semaphore_signal(barrier, inc=1, device_id={"tp": other}, device_id_type=MESH)

    @pl.when(mid)
    def _():
        pl.semaphore_signal(barrier, inc=1, device_id={"tp": cross}, device_id_type=MESH)
        pl.semaphore_wait(barrier, 4)

    @pl.when(jnp.logical_not(mid))
    def _():
        pl.semaphore_wait(barrier, 3)

    def part(d):
        return pl.ds(d * half, half)

    def remote(src, dst, send, recv, dev):
        return pltpu.make_async_remote_copy(
            src_ref=src, dst_ref=dst, send_sem=send, recv_sem=recv, device_id={"tp": dev}, device_id_type=MESH)

    def ag(s, d, p, first=False):
        piece = pl.ds(d * half + p * (half // 2), half // 2)
        src = x_ref.at[piece] if first else xg_ref.at[s - 1, piece]
        k = d * 2 + p
        return remote(src, xg_ref.at[s, piece], ag_send.at[s, k], ag_recv.at[s, k], to[d])

    def skips(s, d):
        r = rho[d]
        return (((r == 0) & (s >= 2) & (s <= 5)) | ((r == 1) & (s >= 4) & (s <= 6))
                | ((r == 3) & (s >= 3) & (s <= 4)))

    def crosses(s, d):
        return mid & (s <= rho[d] + 1)

    def ag_cross(s, d, p, first=False):
        piece = pl.ds(d * half + p * (half // 2), half // 2)
        src = x_ref.at[piece] if first else xg_ref.at[s - 1, piece]
        k = d * 2 + p
        slot = s + 6 - 2 * rho[d]
        return remote(src, xg_ref.at[slot, piece], cs_send.at[s, k], ag_recv.at[slot, k], cross)

    def ag_back(s, d, p):
        piece = pl.ds(d * half + p * (half // 2), half // 2)
        k = d * 2 + p
        return remote(xg_ref.at[s + 1, piece], xg_ref.at[s, piece], bk_send.at[s - 3, k], ag_recv.at[s, k], to[1 - d])

    def taken(s, d):
        return (rho[d] == 1) & (s >= 5) & (s <= 6)

    def xd(s, own=False):
        k = lax.rem(s + RING - 1, RING)
        src = x_ref if own else xg_ref.at[k, pl.ds(0, rows)]
        return remote(src, xg_ref.at[k, pl.ds(rows, rows)], xd_send.at[k], xd_recv.at[k], partner)

    def rsc(s, n, d):
        return remote(sbuf.at[lax.rem(s, 2), n, part(d)], rs.at[lax.rem(s + 1, SLOTS), n, part(d)],
                      rs_send.at[lax.rem(s, 2), n, d], rs_recv.at[lax.rem(s + 1, SLOTS), n, d], to[d])

    def rs_in(s, n, d):
        return remote(sbuf.at[0, n, part(d)], rs.at[lax.rem(s, SLOTS), n, part(d)],
                      rs_send.at[0, n, d], rs_recv.at[lax.rem(s, SLOTS), n, d], to[d])

    def rs_cross(s, n, d):
        return remote(sbuf.at[lax.rem(s, 2), n, part(d)], qb.at[s - 1, n],
                      rs_send.at[lax.rem(s, 2), n, d], q_recv.at[s - 1, n], cross)

    def q_in(s, n):
        return remote(sbuf.at[0, n, part(0)], qb.at[s - 4, n], rs_send.at[0, n, 0], q_recv.at[s - 4, n], cross)

    def dd(s, n):
        slot = lax.rem(s, 2)
        return remote(pbuf.at[n], d2d.at[slot, n], dd_send.at[n], dd_recv.at[slot, n], partner)

    def wgu(i):
        t, slot = lax.rem(i, nf), lax.rem(i, 2)
        cols = pl.ds(pl.multiple_of(t * TF, TF), TF)
        return (pltpu.make_async_copy(wg_ref.at[:, cols], wgbuf.at[slot], wgu_sem.at[slot, 0]),
                pltpu.make_async_copy(wu_ref.at[:, cols], wubuf.at[slot], wgu_sem.at[slot, 1]))

    def wdn(j):
        n, slot = lax.rem(j, nn), lax.rem(j, 2)
        cols = pl.ds(pl.multiple_of(n * TN, TN), TN)
        return pltpu.make_async_copy(wd_ref.at[:, cols], wdbuf.at[slot], wd_sem.at[slot])

    def y_out(n):
        cols = pl.ds(pl.multiple_of(n * TN, TN), TN)
        return pltpu.make_async_copy(sbuf.at[0, n], y_ref.at[:, cols], y_sem.at[n])

    for p in (0, 1):
        for d in (0, 1):
            ag(0, d, p, first=True).start()
    for d in (0, 1):
        @pl.when(rho[d] == 2)
        def _():
            for p in (0, 1):
                ag_cross(0, d, p, first=True).start()
    for copy in wgu(0):
        copy.start()
    wdn(0).start()

    def x_mine(s):
        return pltpu.make_async_copy(xg_ref.at[s - 1, pl.ds(0, rows)], xbuf.at[pl.ds(0, rows)], x_sem.at[0])

    def x_theirs(s):
        k = lax.rem(s + RING - 1, RING)
        return pltpu.make_async_copy(xg_ref.at[k, pl.ds(rows, rows)], xbuf.at[pl.ds(rows, rows)], x_sem.at[1])

    def onward(s, p):
        for d in (0, 1):
            @pl.when(jnp.logical_not(taken(s, d)))
            def _():
                ag(s - 1, d, p, first=True).wait_recv()

            @pl.when((s < RING - 1) & jnp.logical_not(skips(s, d)))
            def _():
                ag(s, d, p).start()

            @pl.when(crosses(s, d) & (rho[d] == 2))
            def _():
                ag_cross(s, d, p).start()

    def arrive(s):
        @pl.when(s > EARLY)
        def _():
            onward(s, 0)
        onward(s, 1)
        xd(s).start()
        x_mine(s).start()
        for d in (0, 1):
            @pl.when((rho[d] == 1) & (s >= 3) & (s <= 4))
            def _():
                for p in (0, 1):
                    ag(s + 1, d, p, first=True).wait_recv()
                    ag_back(s, d, p).start()

            @pl.when((rho[d] == 1) & (s == LATE))
            def _():
                for p in (0, 1):
                    ag_cross(0, d, p, first=True).start()

            @pl.when((rho[d] == 1) & (s > LATE) & (s <= LATE + 2))
            def _():
                for p in (0, 1):
                    ag_cross(s - LATE, d, p).start()

    xd(0, own=True).start()
    pltpu.make_async_copy(x_ref, xbuf.at[pl.ds(0, rows)], x_sem.at[0]).start()
    xd(0, own=True).wait_recv()
    x_theirs(0).start()

    def step(s, carry):
        pltpu.make_async_copy(x_ref, xbuf.at[pl.ds(0, rows)], x_sem.at[0]).wait()
        x_theirs(s).wait()

        def gate_up(t, carry):
            i = s * nf + t

            @pl.when(i + 1 < RING * nf)
            def _():
                for copy in wgu(i + 1):
                    copy.start()
            for copy in wgu(i):
                copy.wait()
            slot = lax.rem(i, 2)

            @pl.when((s < EARLY) & (t == nf - 3))
            def _():
                onward(s + 1, 0)
            gate = jnp.dot(xbuf[...], wgbuf[slot], preferred_element_type=F32)
            up = jnp.dot(xbuf[...], wubuf[slot], preferred_element_type=F32)
            hid[t] = (jax.nn.silu(gate) * up).astype(BF16)
            return carry

        lax.fori_loop(0, nf, gate_up, 0)

        def combine(n):
            k = lax.rem(n, 2)
            dd(s, n).wait_recv()

            @pl.when(s == 0)
            def _():
                own[n] = acc[k] + d2d[lax.rem(s, 2), n].astype(F32)

            for d in (0, 1):
                lines = slice(d * half, (d + 1) * half)

                @pl.when((s > 1) & jnp.logical_not((rho[d] == 3) & (s <= 6)))
                def _():
                    rs_in(s, n, d).wait_recv()
                    acc[k, lines] = acc[k, lines] + rs[lax.rem(s, SLOTS), n, lines].astype(F32)

                @pl.when((rho[d] == 1) & (s >= 4))
                def _():
                    q_in(s, n).wait_recv()
                    acc[k, lines] = acc[k, lines] + qb[s - 4, n].astype(F32)

            @pl.when(s > 2)
            def _():
                for d in (0, 1):
                    rsc(s - 2, n, d).wait_send()

            @pl.when(s > 0)
            def _():
                sbuf[lax.rem(s, 2), n] = (acc[k] + d2d[lax.rem(s, 2), n].astype(F32)).astype(BF16)
                for d in (0, 1):
                    over = (rho[d] == 2) & (s <= 5)

                    @pl.when(over)
                    def _():
                        rs_cross(s, n, d).start()

                    @pl.when(jnp.logical_not(over))
                    def _():
                        rsc(s, n, d).start()

        def down(n, carry):
            j = s * nn + n

            @pl.when(j + 1 < RING * nn)
            def _():
                wdn(j + 1).start()
            wdn(j).wait()
            slot = lax.rem(j, 2)
            term = jnp.dot(hid[0], wdbuf[slot, 0:TF], preferred_element_type=F32)
            for t in range(1, nf):
                term += jnp.dot(hid[t], wdbuf[slot, t * TF:(t + 1) * TF], preferred_element_type=F32)
            acc[lax.rem(n, 2)] = term[:rows]

            @pl.when(s > 0)
            def _():
                dd(s, n).wait_send()
            pbuf[n] = term[rows:].astype(BF16)
            dd(s, n).start()

            @pl.when(n > 0)
            def _():
                combine(n - 1)

            @pl.when((s < RING - 1) & (n == nn - 3))
            def _():
                xd(s + 1).wait_recv()
                x_theirs(s + 1).start()
            return carry

        @pl.when(s < RING - 1)
        def _():
            arrive(s + 1)

        lax.fori_loop(0, nn, down, 0)
        combine(nn - 1)
        return carry

    lax.fori_loop(0, RING, step, 0)

    def finish(n, carry):
        for d in (0, 1):
            rsc(RING - 2, n, d).wait_send()
            rs_in(RING, n, d).wait_recv()
            lines = slice(d * half, (d + 1) * half)

            @pl.when(rho[d] == 1)
            def _():
                q_in(RING, n).wait_recv()
                own[n, lines] = own[n, lines] + qb[RING - 4, n].astype(F32)
        sbuf[0, n] = (own[n] + rs[RING % SLOTS, n].astype(F32)).astype(BF16)
        y_out(n).start()
        return carry

    lax.fori_loop(0, nn, finish, 0)

    def drain(n, carry):
        y_out(n).wait()
        dd(0, n).wait_send()
        for d in (0, 1):
            rsc(RING - 1, n, d).wait_send()
        return carry

    lax.fori_loop(0, nn, drain, 0)
    def sent(s, carry):
        xd(s).wait_send()
        for d in (0, 1):
            for p in (0, 1):
                @pl.when((s < RING - 1) & jnp.logical_not(skips(s, d)))
                def _():
                    ag(s, d, p, first=True).wait_send()

                @pl.when(crosses(s, d))
                def _():
                    ag_cross(s, d, p, first=True).wait_send()

                @pl.when((rho[d] == 1) & (s >= 3) & (s <= 4))
                def _():
                    ag_back(s, d, p).wait_send()
        return carry

    lax.fori_loop(0, RING, sent, 0)


def solution(mesh):
    def step(x, w_gate, w_up, w_down):
        rows, dim = x.shape
        ff = w_gate.shape[1]
        nn = dim // TN
        hbm = pl.BlockSpec(memory_space=pl.ANY)
        dma = pltpu.SemaphoreType.DMA
        out, _ = pl.pallas_call(
            kernel,
            out_shape=(
                jax.ShapeDtypeStruct((rows, dim), BF16),
                jax.ShapeDtypeStruct((RING, 2 * rows, dim), BF16),
            ),
            in_specs=[hbm] * 4,
            out_specs=(hbm, hbm),
            scratch_shapes=[
                pltpu.VMEM((2 * rows, dim), BF16),
                pltpu.VMEM((2, dim, TF), BF16),
                pltpu.VMEM((2, dim, TF), BF16),
                pltpu.VMEM((2, ff, TN), BF16),
                pltpu.VMEM((ff // TF, 2 * rows, TF), BF16),
                pltpu.VMEM((2, rows, TN), F32),
                pltpu.VMEM((nn, rows, TN), F32),
                pltpu.VMEM((SLOTS, nn, rows, TN), BF16),
                pltpu.VMEM((5, nn, rows // 2, TN), BF16),
                pltpu.VMEM((2, nn, rows, TN), BF16),
                pltpu.VMEM((nn, rows, TN), BF16),
                pltpu.VMEM((2, nn, rows, TN), BF16),
                dma((RING, 4)), dma((RING, 4)),
                dma((RING,)), dma((RING,)),
                dma((2, nn, 2)), dma((SLOTS, nn, 2)),
                dma((nn,)), dma((2, nn)),
                dma((2,)), dma((2, 2)), dma((2,)), dma((nn,)),
                dma((4, 4)), dma((2, 4)), dma((5, nn)),
            ],
            compiler_params=pltpu.CompilerParams(
                collective_id=0, has_side_effects=True, vmem_limit_bytes=62 * 1024 * 1024),
        )(x, w_gate, w_up, w_down)
        return out

    return jax.shard_map(
        step,
        mesh=mesh,
        in_specs=(P(("dp", "tp"), None), P(None, "tp"), P(None, "tp"), P("tp", None)),
        out_specs=P(("dp", "tp"), None),
        check_vma=False,
    )
```
